256 devices in a mesh: gx: 256 (over y, z, x, core).
Axes of the slice: x: 4, y: 4, z: 8, core: 2. Of those that a mesh axis runs over, the one named last changes fastest.
Arguments:
- fine: bfloat16 [64, 65536, 128], P(None, 'gx'), may hold values from -6 to 6
- pattern: int32 [8, 65536], P(None, 'gx'), may hold values from 0 to 3
- stencil: bfloat16 [3, 128, 128], replicated, may hold values from -0.3125 to 0.3125
- restrict: bfloat16 [8, 4, 128, 128], replicated, may hold values from -0.5 to 0.5
- coarse_inv: bfloat16 [8, 128, 128], replicated, may hold values from -0.5 to 0.5
Outputs:
- smoothed: float32 [64, 65536, 128], P(None, 'gx')
The draws below stay inside these ranges and needn't reach their ends.
All inputs are finite; a program needn't handle non-finite values.
Results may differ from the reference program's by a relative error of at most 0.0046.
Values may be sent and summed in bfloat16 or wider, within the bound.
A program may use at most 128 MiB of HBM per device.

```python
import jax
import jax.numpy as jnp
from jax import lax

WIDTH = 128
KINDS = 4
LEVELS = 8
BLK_DEV = 256
NVEC = 64
NB = 65536


def touch_ends(values, rng, least, high):
    place = [jax.random.randint(jax.random.fold_in(rng, axis), (), 0, length) for axis, length in enumerate(values.shape)]
    widest = values.shape.index(max(values.shape))
    next_to = place[:widest] + [(place[widest] + 1) % values.shape[widest]] + place[widest + 1:]
    return values.at[tuple(place)].set(least).at[tuple(next_to)].set(high)


def block_levels(key, shape, pieces, low, top_value):
    def one(axis_at, parts):
        steps = jax.random.uniform(jax.random.fold_in(jax.random.fold_in(key, 6), axis_at), (parts,), jnp.float32, low / len(pieces), top_value / len(pieces))
        return jnp.repeat(jnp.exp(steps), shape[axis_at] // parts).reshape((-1,) + (1,) * (len(shape) - axis_at - 1))

    factor_of = one(*pieces[0])
    for cut in pieces[1:]:
        factor_of = factor_of * one(*cut)
    return factor_of


def gaussian(rng, dims, scale, reach, cuts=(), held_as=jnp.bfloat16):
    values = jax.random.normal(rng, dims, jnp.float32) * scale
    if len(cuts) > 0:
        values = block_levels(rng, dims, cuts, -0.22, 0.18) * values
    return jnp.clip(values, min=-reach, max=reach).astype(held_as)


def setup_inputs(seed: int = 0) -> dict:
    key_list = jax.random.split(jax.random.key(seed), 6)
    fine = gaussian(key_list[0], (NVEC, NB, WIDTH), 1.0, 6.0, ((1, 256),))
    pattern = touch_ends(jax.random.randint(key_list[1], (LEVELS, NB), 0, KINDS), jax.random.fold_in(key_list[1], 1), 0, KINDS - 1).astype(jnp.int32)
    stencil = gaussian(key_list[2], (3, WIDTH, WIDTH), (3 * WIDTH) ** -0.5, 0.3125)
    restrict = gaussian(key_list[3], (LEVELS, KINDS, WIDTH, WIDTH), WIDTH ** -0.5, 0.5)
    coarse_inv = gaussian(key_list[4], (LEVELS, WIDTH, WIDTH), WIDTH ** -0.5, 0.5)
    return {"fine": fine, "pattern": pattern, "stencil": stencil, "restrict": restrict, "coarse_inv": coarse_inv}


EXACT = lax.Precision.HIGHEST


def one_vector(fine_vec, pattern, stencil, restrict, coarse_inv):
    all_blocks = fine_vec.shape[0]
    width = fine_vec.shape[1]
    earlier = jnp.roll(fine_vec, 1, axis=0)
    later = jnp.roll(fine_vec, -1, axis=0)
    result = jnp.dot(earlier, stencil[0], preferred_element_type=jnp.float32)
    result = result + jnp.dot(fine_vec, stencil[1], preferred_element_type=jnp.float32)
    result = result + jnp.dot(later, stencil[2], preferred_element_type=jnp.float32)
    widened = fine_vec.astype(jnp.float32)
    kinds_row = jnp.arange(KINDS, dtype=jnp.int32)
    for level_num in range(LEVELS):
        coarse_num = max(all_blocks // 4 ** (level_num + 1), 1)
        span_blocks = all_blocks // coarse_num
        run_len = min(span_blocks, BLK_DEV)
        run_num = all_blocks // run_len
        selector = pattern[level_num][:, None] == kinds_row[None, :]
        onehot = selector.astype(jnp.float32).reshape(run_num, run_len, KINDS)
        tiles = restrict[level_num].astype(jnp.float32)
        grouped = jnp.einsum("nsc,nsk->nkc", widened.reshape(run_num, run_len, width), onehot, precision=EXACT)
        grouped = grouped.astype(jnp.bfloat16).astype(jnp.float32)
        per_run = jnp.einsum("nkc,kcd->nd", grouped, tiles, precision=EXACT)
        coarse = jnp.sum(per_run.reshape(coarse_num, span_blocks // run_len, width), axis=1) * (span_blocks ** -0.5)
        rounded = coarse.astype(jnp.bfloat16)
        solved = jnp.dot(rounded, coarse_inv[level_num], preferred_element_type=jnp.float32).astype(jnp.bfloat16)
        lifted = jnp.einsum("jd,kcd->jkc", solved.astype(jnp.float32), tiles, precision=EXACT)
        kind_map = pattern[level_num].reshape(coarse_num, span_blocks)
        for kind_num in range(KINDS):
            chosen = (kind_map == kind_num)[:, :, None]
            part_add = jnp.where(chosen, lifted[:, kind_num][:, None, :], jnp.float32(0.0))
            result = result + part_add.reshape(all_blocks, width)
    return result


def reference(fine, pattern, stencil, restrict, coarse_inv):
    return lax.map(lambda fine_vec: one_vector(fine_vec, pattern, stencil, restrict, coarse_inv), fine)
```

```python
import functools

import jax
import jax.numpy as jnp
from jax import lax
from jax.experimental import pallas as pl
from jax.experimental.pallas import tpu as pltpu
from jax.sharding import PartitionSpec as P

F32, BF16, I32 = jnp.float32, jnp.bfloat16, jnp.int32
MESH = pl.DeviceIdType.MESH
NV, BLK, W, KINDS, LEVELS = 64, 256, 128, 4, 8
CH = 8
GP = 40
LP = 24


def dot(a, b):
    return jnp.dot(a, b, preferred_element_type=F32)


def dot_t(a, b):
    return lax.dot_general(a, b, (((1,), (1,)), ((), ())), preferred_element_type=F32)


def iota(shape, dim):
    return lax.broadcasted_iota(I32, shape, dim)


def main_kernel(fine, pattern, stencil, tiles, inverse, p_out, rt_out, st_out,
                fbuf, pat, wst, wr, wc, sel, spread, tt, wpair, gl1, gl2, gs, cb, sb, lb1, lb2, ls, ext,
                pscr, asend, arecv, bsend, brecv, b6send, b6recv, ysend, yrecv, csend, crecv, solved, hsend, hrecv,
                f_sem, w_sem, a_ssem, a_rsem, b_ssem, b_rsem, b6_ssem, b6_rsem, y_ssem, y_rsem, c_ssem, c_rsem, h_ssem, h_rsem):
    me = lax.axis_index("gx")
    n = 256
    q = lax.rem(me, 8)
    base = me - q
    z = lax.rem(lax.div(me, 8), 8)
    y = lax.div(me, 64)
    rest = lax.rem(me, 64)
    q_peer = [base + (q ^ d) for d in range(8)]
    z_peer = [me - 8 * z + 8 * (z ^ d) for d in range(8)]
    y_peer = [64 * (y ^ d) + rest for d in range(4)]
    after, before = lax.rem(me + 1, n), lax.rem(me + n - 1, n)

    barrier = pltpu.get_barrier_semaphore()
    greet = q_peer[1:] + z_peer[1:] + y_peer[1:] + [after, before]
    for peer in greet:
        pl.semaphore_signal(barrier, inc=1, device_id=(peer,), device_id_type=MESH)

    def small(src, dst, k):
        return pltpu.make_async_copy(src, dst, w_sem.at[k])

    loads = [small(pattern, pat, 0), small(tiles, wr, 1), small(stencil, wst, 2), small(inverse, wc, 3)]
    loads[0].start()

    def chunk(c):
        at = pl.ds(c * CH, CH)
        return pltpu.make_async_copy(fine.at[at], fbuf.at[at], f_sem.at[c])

    for c in range(NV // CH):
        chunk(c).start()
    for copy in loads[1:]:
        copy.start()
    loads[0].wait()

    col = iota((1, BLK), 1)
    rows = []
    for l in range(1, LEVELS + 1):
        kind = pat[l - 1:l, :]
        if l == 1:
            rows.append(kind * 64 + lax.shift_right_logical(col, 2))
        elif l == 2:
            rows.append(kind * 16 + lax.shift_right_logical(col, 4) + 256)
        elif l == 3:
            rows.append(kind * 4 + lax.shift_right_logical(col, 6) + 320)
        else:
            rows.append(kind + (336 + 4 * (l - 4)))
    r1 = iota((256, BLK), 0)
    sel[0:256, :] = jnp.where(r1 == rows[0], 1.0, 0.0).astype(BF16)
    r2 = iota((112, BLK), 0) + 256
    c2 = iota((112, BLK), 1)
    hit = ((r2 == 356) & (c2 == 0)) | ((r2 == 357) & (c2 == BLK - 1))
    for row in rows[1:]:
        hit = hit | (r2 == row)
    sel[256:368, :] = jnp.where(hit, 1.0, 0.0).astype(BF16)

    target = jnp.concatenate([jnp.concatenate(rows, axis=0).astype(F32), jnp.zeros((120, BLK), F32)], axis=0)
    tt[...] = jnp.transpose(target)

    def gather(c, carry):
        chunk(c).wait()
        for p in range(CH // 2):
            v = c * CH + 2 * p
            g = dot(sel[...], jnp.concatenate([fbuf[v], fbuf[v + 1]], axis=1))
            for h in range(2):
                lanes = slice(h * W, (h + 1) * W)
                u = v + h
                for k in range(KINDS):
                    gl1[k, pl.ds(pl.multiple_of(u * 64, 64), 64), :] = g[k * 64:(k + 1) * 64, lanes].astype(BF16)
                    gl2[k, pl.ds(pl.multiple_of(u * 16, 16), 16), :] = g[256 + k * 16:256 + (k + 1) * 16, lanes].astype(BF16)
                gs[pl.ds(pl.multiple_of(u * GP, 8), GP), :] = g[320:360, lanes]
        return carry

    lax.fori_loop(0, NV // CH, gather, 0)

    def of_row(r):
        return gs[pl.ds(r, NV, stride=GP), :]

    hsend[0] = of_row(36).astype(BF16)
    hsend[1] = of_row(37).astype(BF16)
    for copy in loads[1:]:
        copy.wait()
    for s in range(4):
        l = 4 + s
        x = jnp.concatenate([of_row(20 + 4 * s + k) for k in range(KINDS)], axis=1).astype(BF16)
        pscr[s] = dot(x, wr[l]) * (2.0 ** -(l + 1))
    for d in range(8):
        at = pl.ds(pl.multiple_of(8 * (q ^ d), 8), 8)
        part = jnp.concatenate([pscr[s, at, :] for s in range(4)], axis=0).astype(BF16)
        asend[d] = part

    pl.semaphore_wait(barrier, len(greet))

    def remote(src, dst, ssem, rsem, peer):
        return pltpu.make_async_remote_copy(src_ref=src, dst_ref=dst, send_sem=ssem, recv_sem=rsem,
                                            device_id=(peer,), device_id_type=MESH)

    a_copies = [remote(asend.at[d], arecv.at[d], a_ssem.at[d], a_rsem.at[d], q_peer[d]) for d in range(1, 8)]
    for copy in a_copies:
        copy.start()
    h_copies = [remote(hsend.at[0], hrecv.at[0], h_ssem.at[0], h_rsem.at[0], before),
                remote(hsend.at[1], hrecv.at[1], h_ssem.at[1], h_rsem.at[1], after)]
    for copy in h_copies:
        copy.start()

    tt_even = tt[pl.ds(0, 128, stride=2), :]
    tt_odd = tt[pl.ds(1, 128, stride=2), :]
    for half, t in enumerate((tt_even, tt_odd)):
        lane = iota((128, 128), 1)
        sub = iota((128, 128), 0)
        at = slice(half * 128, (half + 1) * 128)
        t1 = t[:, 0:1].astype(I32)
        spread[0, at, :] = jnp.where(lane == t1, 1.0, 0.0).astype(BF16)
        spread[1, at, :] = jnp.where(lane + 128 == t1, 1.0, 0.0).astype(BF16)
        hit = (lane + 256 == t[:, 1:2].astype(I32)) | (lane + 256 == t[:, 2:3].astype(I32)) | (lane + 256 == t[:, 3:4].astype(I32))
        hit = hit & (lane < 84)
        if half == 0:
            hit = hit | ((sub == 0) & ((lane == 84) | (lane == 85)))
        else:
            hit = hit | ((sub == 127) & ((lane == 86) | (lane == 87)))
        spread[2, at, :] = jnp.where(hit, 1.0, 0.0).astype(BF16)
    lane = iota((BLK, 128), 1)
    hit = lane < 0
    for s in range(4):
        hit = hit | (lane + 340 == tt[:, 4 + s:5 + s].astype(I32))
    st_out[...] = jnp.where(hit, 1.0, 0.0).astype(BF16)

    zero = jnp.zeros((W, W), BF16)
    w0, w1, w2 = wst[0], wst[1], wst[2]
    wpair[0:128, :] = jnp.concatenate([w1, w0], axis=1)
    wpair[128:256, :] = jnp.concatenate([w2, w1], axis=1)
    wpair[256:384, :] = jnp.concatenate([w0, zero], axis=1)
    wpair[384:512, :] = jnp.concatenate([zero, w2], axis=1)
    ls[...] = jnp.zeros_like(ls)
    for slot in range(2):
        ext[slot, 0:8, :] = jnp.zeros((8, W), F32)
        ext[slot, 264:272, :] = jnp.zeros((8, W), F32)

    def solve(c, l):
        return dot(c.astype(BF16), wc[l]).astype(BF16)

    for l, first, j_num in ((2, 0, 4), (3, 16, 1)):
        for j in range(j_num):
            x = jnp.concatenate([of_row(first + j_num * k + j) for k in range(KINDS)], axis=1).astype(BF16)
            s = solve(dot(x, wr[l]) * (2.0 ** -(l + 1)), l)
            lifted = dot_t(s, wr[l])
            for k in range(KINDS):
                ls[pl.ds(first + j_num * k + j, NV, stride=LP), :] = lifted[:, k * W:(k + 1) * W]

    def level2(i, carry):
        at = pl.ds(pl.multiple_of(i * 256, 256), 256)
        x = jnp.concatenate([gl2[k, at, :] for k in range(KINDS)], axis=1)
        s = solve(dot(x, wr[1]) * 0.25, 1)
        lifted = dot_t(s, wr[1]).astype(BF16)
        for u in range(16):
            for k in range(KINDS):
                lb2[i * 16 + u, k * 16:(k + 1) * 16, :] = lifted[u * 16:(u + 1) * 16, k * W:(k + 1) * W]
        return carry

    lax.fori_loop(0, NV // 16, level2, 0)

    for copy in h_copies:
        copy.wait()
    for side, tile in ((1, 0), (0, 2)):
        at = 20 if side == 1 else 22
        add = dot(hrecv[side], wst[tile])
        high = add.astype(BF16).astype(F32)
        ls[pl.ds(at, NV, stride=LP), :] = high
        ls[pl.ds(at + 1, NV, stride=LP), :] = add - high

    def restrict1(i):
        at = pl.ds(pl.multiple_of(i * 256, 256), 256)
        x = jnp.concatenate([gl1[k, at, :] for k in range(KINDS)], axis=1)
        cb[at, :] = (dot(x, wr[0]) * 0.5).astype(BF16)

    def solve1(i):
        at = pl.ds(pl.multiple_of(i * 256, 256), 256)
        sb[at, :] = dot(cb[at, :], wc[0]).astype(BF16)

    def lift1(i):
        at = pl.ds(pl.multiple_of(i * 256, 256), 256)
        lifted = dot_t(sb[at, :], wr[0]).astype(BF16)
        for u in range(4):
            for k in range(KINDS):
                lb1[i * 4 + u, k * 64:(k + 1) * 64, :] = lifted[u * 64:(u + 1) * 64, k * W:(k + 1) * W]

    def local(i):
        for p in range(2):
            v = i * 4 + p * 2
            parts = []
            for h in range(2):
                u = v + h
                little = ls[pl.ds(pl.multiple_of(u * LP, 8), 32), :].astype(BF16)
                parts.append(jnp.concatenate([lb1[u], lb2[u], little, jnp.zeros((32, W), BF16)], axis=0))
            m = jnp.concatenate([spread[0], spread[1], spread[2]], axis=1)
            out = dot(m, jnp.concatenate(parts, axis=1))
            for h in range(2):
                u = v + h
                e = ext.at[h]
                e[8:264, :] = fbuf[u].astype(F32)
                x = jnp.concatenate([e[pl.ds(8, 128, stride=2), :], e[pl.ds(9, 128, stride=2), :],
                                     e[pl.ds(7, 128, stride=2), :], e[pl.ds(10, 128, stride=2), :]], axis=1).astype(BF16)
                near = dot(x, wpair[...])
                lanes = slice(h * W, (h + 1) * W)
                o = p_out.at[u]
                o[pl.ds(0, 128, stride=2), :] = out[0:128, lanes] + near[:, 0:128]
                o[pl.ds(1, 128, stride=2), :] = out[128:256, lanes] + near[:, 128:256]

    def step(i, carry):
        restrict1(jnp.minimum(i, 15))
        solve1(jnp.clip(i - 1, 0, 15))
        lift1(jnp.clip(i - 2, 0, 15))
        local(jnp.clip(i - 3, 0, 15))
        return carry

    lax.fori_loop(0, 3, step, 0)

    for copy in a_copies:
        copy.wait()
    near = asend[0].astype(F32)
    for d in range(1, 4):
        near = near + arecv[d].astype(F32)
    far = arecv[4].astype(F32)
    for d in range(5, 8):
        far = far + arecv[d].astype(F32)
    total = near + far
    bsend[...] = total[16:32].astype(BF16)
    b6send[...] = total[0:16].astype(BF16)
    b_copies = [remote(bsend, brecv.at[d], b_ssem.at[d], b_rsem.at[d], z_peer[d]) for d in range(1, 8)]
    b_copies.append(remote(b6send, b6recv, b6_ssem, b6_rsem, z_peer[1]))
    for copy in b_copies:
        copy.start()
    five_near = solve(near[0:8], 4)
    five_far = solve(far[0:8], 4)

    lax.fori_loop(3, 9, step, 0)

    for copy in b_copies:
        copy.wait()
    total = bsend[...].astype(F32)
    for d in range(1, 8):
        total = total + brecv[d].astype(F32)
    ysend[...] = total[8:16]
    y_copies = [remote(ysend, yrecv.at[d], y_ssem.at[d], y_rsem.at[d], y_peer[d]) for d in range(1, 4)]
    for copy in y_copies:
        copy.start()
    six = solve(b6send[...].astype(F32)[8:16] + b6recv[...].astype(F32)[8:16], 5)
    seven = solve(total[0:8], 6)

    lax.fori_loop(9, 14, step, 0)

    for copy in y_copies:
        copy.wait()
    eight = ysend[...]
    for d in range(1, 4):
        eight = eight + yrecv[d]
    eight = solve(eight, 7)
    csend[0] = jnp.concatenate([s.astype(F32) for s in (five_near, six, seven, eight)], axis=0).astype(BF16)
    csend[1] = jnp.concatenate([s.astype(F32) for s in (five_far, six, seven, eight)], axis=0).astype(BF16)
    c_copies = [remote(csend.at[d // 4], crecv.at[d], c_ssem.at[d], c_rsem.at[d], q_peer[d]) for d in range(1, 8)]
    for copy in c_copies:
        copy.start()

    lax.fori_loop(14, 19, step, 0)

    for copy in c_copies:
        copy.wait()
    for d in range(8):
        block = (csend[0] if d == 0 else crecv[d]).astype(F32)
        at = pl.ds(pl.multiple_of(8 * (q ^ d), 8), 8)
        for s in range(4):
            solved[s, at, :] = block[8 * s:8 * s + 8]
    for s in range(4):
        lifted = dot_t(solved[s].astype(BF16), wr[4 + s])
        for k in range(KINDS):
            rt_out[pl.ds(4 * s + k, NV, stride=LP), :] = lifted[:, k * W:(k + 1) * W]


def add_kernel(p_ref, rt, st, out, buf, sem):
    def copy(c):
        at = pl.ds(c * 4, 4)
        return pltpu.make_async_copy(buf.at[at], out.at[at], sem.at[c])

    m = st[:, 0:16]

    def step(c, carry):
        for p in range(2):
            v = c * 4 + 2 * p
            rhs = jnp.concatenate([rt[pl.ds(pl.multiple_of((v + h) * LP, 8), 16), :].astype(BF16) for h in range(2)], axis=1)
            add = dot(m, rhs)
            for h in range(2):
                buf[v + h] = p_ref[v + h] + add[:, h * W:(h + 1) * W]
        copy(c).start()
        return carry

    lax.fori_loop(0, NV // 4, step, 0)

    def wait(c, carry):
        copy(c).wait()
        return carry

    lax.fori_loop(0, NV // 4, wait, 0)


def shards(fine, pattern, stencil, restrict, coarse_inv):
    any_spec = pl.BlockSpec(memory_space=pltpu.HBM)
    vmem_spec = pl.BlockSpec(memory_space=pltpu.VMEM)
    dma = pltpu.SemaphoreType.DMA
    V = pltpu.VMEM
    tiles = restrict.reshape(LEVELS, KINDS * W, W)
    partial, rt, st = pl.pallas_call(
        main_kernel,
        out_shape=(V((NV, BLK, W), F32), V((NV * LP, W), F32), V((BLK, 128), BF16)),
        in_specs=[any_spec] * 5,
        out_specs=(vmem_spec, vmem_spec, vmem_spec),
        scratch_shapes=[
            V((NV, BLK, W), BF16), V((LEVELS, BLK), I32), V((3, W, W), BF16), V((LEVELS, KINDS * W, W), BF16), V((LEVELS, W, W), BF16),
            V((368, BLK), BF16), V((3, BLK, 128), BF16), V((BLK, 128), F32), V((512, 256), BF16),
            V((KINDS, NV * 64, W), BF16), V((KINDS, NV * 16, W), BF16), V((NV * GP, W), F32),
            V((NV * 64, W), BF16), V((NV * 64, W), BF16), V((NV, 256, W), BF16), V((NV, 64, W), BF16), V((NV * LP + 8, W), F32),
            V((2, 272, W), F32),
            V((4, NV, W), F32), V((8, 32, W), BF16), V((8, 32, W), BF16), V((16, W), BF16), V((8, 16, W), BF16),
            V((16, W), BF16), V((16, W), BF16), V((8, W), F32), V((4, 8, W), F32), V((2, 32, W), BF16), V((8, 32, W), BF16),
            V((4, NV, W), F32), V((2, NV, W), BF16), V((2, NV, W), BF16),
            dma((NV // CH,)), dma((4,)), dma((8,)), dma((8,)), dma((8,)), dma((8,)), dma, dma, dma((4,)), dma((4,)),
            dma((8,)), dma((8,)), dma((2,)), dma((2,)),
        ],
        compiler_params=pltpu.CompilerParams(collective_id=0, has_side_effects=True, vmem_limit_bytes=44 << 20),
        name="multilevel",
    )(fine, pattern, stencil, tiles, coarse_inv)
    return pl.pallas_call(
        add_kernel,
        out_shape=jax.ShapeDtypeStruct((NV, BLK, W), F32),
        in_specs=[vmem_spec] * 3,
        out_specs=any_spec,
        scratch_shapes=[V((NV, BLK, W), F32), dma((NV // 4,))],
        compiler_params=pltpu.CompilerParams(vmem_limit_bytes=24 << 20),
        name="add_coarse",
    )(partial, rt, st)


def solution(mesh):
    in_specs = (P(None, "gx", None), P(None, "gx"), P(), P(), P())
    return jax.shard_map(shards, mesh=mesh, in_specs=in_specs, out_specs=P(None, "gx", None), check_vma=False)
```
